128 devices in a mesh: group: 2 (over z_hi), slab: 64 (over y, x, z_lo, core).
Axes of the slice: x: 4, y: 4, z: 4 (z_hi: 2, z_lo: 2; z = z_hi * 2 + z_lo), core: 2. Of those that a mesh axis runs over, the one named last changes fastest.
Arguments:
- queries: bfloat16 [65536, 512], P(('group', 'slab')), may hold values from -6 to 6
- keys: bfloat16 [65536, 512], P(('group', 'slab')), may hold values from -6 to 6
- values: bfloat16 [65536, 512], P(('group', 'slab')), may hold values from -6 to 6
- neighbours: int32 [512, 6], P(('group', 'slab')), may hold values from 0 to 15, as said below
- live_tiles: int32 [128], P(('group', 'slab')), may hold values from 1 to 4, as said below
- boundary_ids: int32 [128, 4], P(('group', 'slab')), may hold values from 0 to 3, as said below
Outputs:
- attended: bfloat16 [65536, 512], P(('group', 'slab'))
The draws below stay inside these ranges and needn't reach their ends.
Inputs may be any that keep to these rules, and one draw needn't show every extreme that they name: `neighbours`: each row names 6 different positions of the pool. `live_tiles`: some slab has all 4 tiles active. `boundary_ids`: each row names 4 different tiles of its slab.
All inputs are finite; a program needn't handle non-finite values.
Results may differ from the reference program's by a relative error of at most 0.008.
Values may be sent and summed in bfloat16 or wider, within the bound.
No kernel may reach another device: no remote copies, remote signals or barrier semaphores. Data moves between devices by JAX's collectives and lax.ppermute only.
A program may use at most 128 MiB of HBM per device.

```python
import jax
import jax.numpy as jnp
from jax import lax

HEADS = 8
HEAD_DIM = 64
TILE = 128
TILES_DEV = 4
HALO = 4
BOUNDARY = 4
LISTED = 6
BLOCK = 4
POOL = 16
NTILES = 512
NODES = 65536
N_GROUP = 2
N_SLAB = 64
DEVICES = 128


def draw_queries(key, part):
    width = HEADS * HEAD_DIM
    base = jax.random.normal(jax.random.fold_in(key, 11), (NODES, width), jnp.float32)
    return jnp.clip(base, -6.0, 6.0).astype(jnp.bfloat16)


def draw_keys(key, part):
    width = HEADS * HEAD_DIM
    base = jax.random.normal(jax.random.fold_in(key, 17), (NODES, width), jnp.float32)
    return jnp.clip(base, -6.0, 6.0).astype(jnp.bfloat16)


def draw_neighbours(key, part):
    row_keys = jax.random.split(jax.random.fold_in(key, 23), NTILES)
    picked = jax.vmap(lambda row_key: jax.random.permutation(row_key, POOL)[:LISTED])(row_keys)
    return picked.astype(jnp.int32)


def draw_live_tiles(key, part):
    counts = jax.random.randint(jax.random.fold_in(key, 29), (DEVICES,), 1, TILES_DEV + 1)
    fullest = jax.random.randint(jax.random.fold_in(key, 31), (), 0, DEVICES)
    return counts.at[fullest].set(TILES_DEV).astype(jnp.int32)


def draw_boundary_ids(key, part):
    row_keys = jax.random.split(jax.random.fold_in(key, 37), DEVICES)
    picked = jax.vmap(lambda row_key: jax.random.permutation(row_key, TILES_DEV)[:BOUNDARY])(row_keys)
    return picked.astype(jnp.int32)


def steps_of(rng, extent, cuts, low, high):
    loudness = 1.0
    for axis_at, shards_of in cuts:
        steps = jax.random.uniform(jax.random.fold_in(jax.random.fold_in(rng, 6), axis_at), (shards_of,), jnp.float32, low / len(cuts), high / len(cuts))
        loudness = loudness * jnp.repeat(jnp.exp(steps), extent[axis_at] // shards_of).reshape((-1,) + (1,) * (len(extent) - 1 - axis_at))
    return loudness


def bell_draw(own_key, shape, scale, bound, cuts=(), held_as=jnp.bfloat16):
    values = scale * jax.random.normal(own_key, shape, jnp.float32)
    if cuts:
        values = values * steps_of(own_key, shape, cuts, -0.22, 0.18)
    return jnp.clip(values, -bound, bound).astype(held_as)


def setup_inputs(seed: int = 0) -> dict:
    splits = jax.random.split(jax.random.key(seed), 7)
    return {
        "queries": draw_queries(jax.random.fold_in(splits[6], 71), 0),
        "keys": draw_keys(jax.random.fold_in(splits[6], 71), 0),
        "values": bell_draw(splits[2], (NODES, HEADS * HEAD_DIM), 1.0, 6.0, ((0, 128),)),
        "neighbours": draw_neighbours(jax.random.fold_in(splits[6], 71), 0),
        "live_tiles": draw_live_tiles(jax.random.fold_in(splits[6], 71), 0),
        "boundary_ids": draw_boundary_ids(jax.random.fold_in(splits[6], 71), 0),
    }


def attend(tile_queries, pool, lists, live):
    width = HEADS * HEAD_DIM

    def one_block(number):
        start = (number * BLOCK).astype(jnp.int32)
        query_block = lax.dynamic_slice_in_dim(tile_queries, start, BLOCK, 0)
        chosen = lax.dynamic_slice_in_dim(lists, start, BLOCK, 0)
        key_set = pool[0][chosen].reshape(BLOCK, LISTED * TILE, HEADS, HEAD_DIM)
        value_set = pool[1][chosen].reshape(BLOCK, LISTED * TILE, HEADS, HEAD_DIM)
        query_set = query_block.reshape(BLOCK, TILE, HEADS, HEAD_DIM)
        scores = jnp.einsum("qihd,qjhd->qhij", query_set.astype(jnp.float32), key_set.astype(jnp.float32)) * (HEAD_DIM ** -0.5)
        weights = jax.nn.softmax(scores, axis=-1).astype(jnp.bfloat16)
        mixed = jnp.einsum("qhij,qjhd->qihd", weights.astype(jnp.float32), value_set.astype(jnp.float32))
        alive = (start + jnp.arange(BLOCK, dtype=jnp.int32)) < live
        mixed = jnp.where(alive[:, None, None, None], mixed, 0.0)
        return mixed.astype(jnp.bfloat16).reshape(BLOCK, TILE, width)

    outputs = lax.map(one_block, jnp.arange(TILES_DEV // BLOCK, dtype=jnp.int32))
    return outputs.reshape(TILES_DEV * TILE, width)


def reference(queries, keys, values, neighbours, live_tiles, boundary_ids):
    width = HEADS * HEAD_DIM
    regions = N_GROUP
    slabs = N_SLAB
    pairs = jnp.stack([keys, values]).reshape(2, regions, slabs, TILES_DEV, TILE, width)
    query_tiles = queries.reshape(regions * slabs, TILES_DEV, TILE, width)
    lists = neighbours.reshape(regions * slabs, TILES_DEV, LISTED)
    borders = boundary_ids.reshape(regions, slabs, BOUNDARY)

    def one_slab(index):
        region = index // slabs
        within = index % slabs
        own_tiles = pairs[:, region, within]
        before = pairs[:, region, (within - 1) % slabs][:, TILES_DEV - HALO:]
        after = pairs[:, region, (within + 1) % slabs][:, :HALO]
        source = (region - 1) % regions
        remote = pairs[:, source, within]
        border = jnp.take(remote, borders[source, within], axis=1)
        pool = jnp.concatenate([own_tiles, before, after, border], axis=1)
        return attend(query_tiles[index], pool, lists[index], live_tiles[index])

    result = lax.map(one_slab, jnp.arange(regions * slabs, dtype=jnp.int32))
    return result.reshape(NODES, width)
```

```python
import math

import jax
import jax.numpy as jnp
from jax import lax
from jax.experimental import pallas as pl
from jax.experimental.pallas import tpu as pltpu
from jax.sharding import PartitionSpec as P


HEADS = 8
HEAD_DIM = 64
TILE = 128
TILES = 4
LISTED = 6
PAIRS = 4
BATCH = 4
WIDTH = HEADS * HEAD_DIM
AXES = ("group", "slab")
SCALE = HEAD_DIM ** (-0.5) * math.log2(math.e)
LOWEST = -1e30

VMEM = pl.BlockSpec(memory_space=pltpu.VMEM)
SMEM = pl.BlockSpec(memory_space=pltpu.SMEM)


def move(block, target):
    groups, slabs = lax.axis_size("group"), lax.axis_size("slab")
    route = []
    for g in range(groups):
        for s in range(slabs):
            to_g, to_s = target(g, s)
            route.append((g * slabs + s, (to_g % groups) * slabs + to_s % slabs))
    return lax.ppermute(block, AXES, route)


def to_chip(g, s):
    return g, s ^ 1


def to_cross(g, s):
    return g, s ^ 3


def to_forward(g, s):
    return 1 - g, s ^ 3


def to_along(g, s):
    return g, (s + 4 if s % 2 == 0 else s - 4)


def to_group(g, s):
    return 1 - g, s


def prepare_kernel(q_ref, v_ref, w_ref, v_out):
    for t in range(TILES):
        rows = pl.ds(t * TILE, TILE)
        for p in range(PAIRS):
            lanes = pl.ds(p * TILE, TILE)
            v_out[rows, lanes] = v_ref[rows, lanes].T
            qt = q_ref[rows, lanes].T
            zero = jnp.zeros((HEAD_DIM, TILE), jnp.bfloat16)
            w_ref[t, p, :HEAD_DIM, :TILE] = qt[:HEAD_DIM]
            w_ref[t, p, :HEAD_DIM, TILE:] = zero
            w_ref[t, p, HEAD_DIM:, :TILE] = zero
            w_ref[t, p, HEAD_DIM:, TILE:] = qt[HEAD_DIM:]


def prepare(q, v):
    return pl.pallas_call(
        prepare_kernel,
        out_shape=(
            jax.ShapeDtypeStruct((TILES, PAIRS, TILE, 2 * TILE), jnp.bfloat16),
            jax.ShapeDtypeStruct(v.shape, jnp.bfloat16),
        ),
        in_specs=[VMEM, VMEM],
        out_specs=(VMEM, VMEM),
        compiler_params=pltpu.CompilerParams(vmem_limit_bytes=8 << 20),
        cost_estimate=pl.CostEstimate(flops=10**6, bytes_accessed=3 << 20, transcendentals=0),
        name="prepare",
    )(q, v)


def list_items(lists_ref, live, source_of, items):
    count = jnp.int32(0)
    for t in range(TILES):
        for j in range(LISTED):
            here, tile = source_of(lists_ref[t, j])
            items[count] = t * 16 + tile
            count = count + jnp.where(jnp.logical_and(here, t < live), 1, 0)
    for j in range(BATCH - 1):
        items[count + j] = TILES * 16
    return lax.div(count + (BATCH - 1), jnp.int32(BATCH))


def attend_items(batches, items, k_ref, v_ref, w_ref, acc, peak, total):
    def batch(b, carry):
        for u in range(BATCH):
            item = items[b * BATCH + u]
            t = lax.div(item, jnp.int32(16))
            rows = pl.ds(pl.multiple_of(lax.rem(item, jnp.int32(16)) * TILE, TILE), TILE)
            tq = jnp.minimum(t, TILES - 1)
            tops, sums, mixes = [], [], []
            for p in range(PAIRS):
                lanes = pl.ds(p * TILE, TILE)
                scores = jnp.dot(k_ref[rows, lanes], w_ref[tq, p], preferred_element_type=jnp.float32)
                top = jnp.max(scores, axis=0, keepdims=True)
                weights = jnp.exp2(scores * SCALE - top * SCALE)
                add = jnp.sum(weights, axis=0, keepdims=True)
                weights = weights.astype(jnp.bfloat16)
                vt = v_ref[rows, lanes]
                for h in range(2):
                    half = slice(h * TILE, (h + 1) * TILE)
                    tops.append(top[:, half])
                    sums.append(add[:, half])
                    mixes.append(
                        jnp.dot(
                            vt[h * HEAD_DIM : (h + 1) * HEAD_DIM],
                            weights[:, half],
                            preferred_element_type=jnp.float32,
                        )
                    )
            top = jnp.concatenate(tops, axis=0)
            add = jnp.concatenate(sums, axis=0)
            old = peak[t]
            new = jnp.maximum(old, top)
            keep = jnp.exp2((old - new) * SCALE)
            take = jnp.exp2((top - new) * SCALE)
            peak[t] = new
            total[t] = total[t] * keep + add * take
            for h in range(HEADS):
                dims = pl.ds(h * HEAD_DIM, HEAD_DIM)
                acc[t, dims] = acc[t, dims] * keep[h : h + 1] + mixes[h] * take[h : h + 1]
        return carry

    lax.fori_loop(0, batches, batch, 0)


def first_kernel(lists, live, k_ref, v_ref, w_ref, acc, peak, total, items):
    acc[...] = jnp.zeros_like(acc)
    peak[...] = jnp.full_like(peak, LOWEST)
    total[...] = jnp.zeros_like(total)
    batches = list_items(lists, live[0], lambda pos: (pos < TILES, lax.rem(pos, 4)), items)
    attend_items(batches, items, k_ref, v_ref, w_ref, acc, peak, total)


STATE = (
    jax.ShapeDtypeStruct((TILES + 1, WIDTH, TILE), jnp.float32),
    jax.ShapeDtypeStruct((TILES + 1, HEADS, TILE), jnp.float32),
    jax.ShapeDtypeStruct((TILES + 1, HEADS, TILE), jnp.float32),
)
ITEMS = pltpu.SMEM((TILES * LISTED + BATCH,), jnp.int32)


def flops(items):
    return pl.CostEstimate(flops=items * 40_000_000, bytes_accessed=1 << 20, transcendentals=0)


def first_stage(lists, live, k, v, w):
    return pl.pallas_call(
        first_kernel,
        out_shape=STATE,
        in_specs=[SMEM, SMEM] + [VMEM] * 3,
        out_specs=(VMEM,) * 3,
        scratch_shapes=[ITEMS],
        compiler_params=pltpu.CompilerParams(vmem_limit_bytes=16 << 20),
        cost_estimate=flops(8),
        name="first_stage",
    )(lists, live, k, v, w)


def pool_half(half, odd):
    def source_of(ids_ref):
        def find(pos):
            other = jnp.where(odd, 2 * TILES, TILES)
            beside = pos - other
            is_beside = jnp.logical_and(beside >= 2 * half, beside < 2 * half + 2)
            far = ids_ref[0, jnp.maximum(pos - 3 * TILES, 0)] - 2 * half
            is_far = jnp.logical_and(pos >= 3 * TILES, jnp.logical_and(far >= 0, far < 2))
            tile = jnp.where(is_beside, beside - 2 * half, jnp.where(is_far, far + 2, 0))
            return jnp.logical_or(is_beside, is_far), tile

        return find

    return source_of


def pick(inner, refs, k_all, v_all):
    kb, vb, kd, vd, kc, vc = refs

    @pl.when(inner)
    def _():
        k_all[: 2 * TILE] = kb[...]
        v_all[: 2 * TILE] = vb[...]

    @pl.when(jnp.logical_not(inner))
    def _():
        k_all[: 2 * TILE] = kd[...]
        v_all[: 2 * TILE] = vd[...]

    k_all[2 * TILE :] = kc[...]
    v_all[2 * TILE :] = vc[...]


def middle_kernel(lists, live, ids, slab, kn, vn, kb, vb, kd, vd, kc, vc, w_ref, acc0, peak0, total0, acc, peak, total, items, k_all, v_all):
    odd = lax.rem(slab[0], 2) == 1
    inner = jnp.logical_or(lax.rem(slab[0], 4) == 1, lax.rem(slab[0], 4) == 2)

    def near(pos):
        at = pos - jnp.where(odd, TILES, 2 * TILES)
        here = jnp.logical_and(at >= 0, at < TILES)
        return here, jnp.where(here, at, 0)

    batches = list_items(lists, live[0], near, items)
    attend_items(batches, items, kn, vn, w_ref, acc, peak, total)
    pick(inner, (kb, vb, kd, vd, kc, vc), k_all, v_all)
    batches = list_items(lists, live[0], pool_half(0, odd)(ids), items)
    attend_items(batches, items, k_all, v_all, w_ref, acc, peak, total)


def middle_stage(lists, live, ids, slab, tiles, w, state):
    return pl.pallas_call(
        middle_kernel,
        out_shape=STATE,
        in_specs=[SMEM] * 4 + [VMEM] * 12,
        out_specs=(VMEM,) * 3,
        input_output_aliases={13: 0, 14: 1, 15: 2},
        scratch_shapes=[ITEMS, pltpu.VMEM((4 * TILE, WIDTH), jnp.bfloat16), pltpu.VMEM((4 * TILE, WIDTH), jnp.bfloat16)],
        compiler_params=pltpu.CompilerParams(vmem_limit_bytes=20 << 20),
        cost_estimate=flops(16),
        name="middle_stage",
    )(lists, live, ids, slab, *tiles, w, *state)


def last_kernel(lists, live, ids, slab, kb, vb, kd, vd, kc, vc, w_ref, acc, peak, total, out, items, k_all, v_all):
    odd = lax.rem(slab[0], 2) == 1
    inner = jnp.logical_or(lax.rem(slab[0], 4) == 1, lax.rem(slab[0], 4) == 2)
    pick(inner, (kb, vb, kd, vd, kc, vc), k_all, v_all)
    batches = list_items(lists, live[0], pool_half(1, odd)(ids), items)
    attend_items(batches, items, k_all, v_all, w_ref, acc, peak, total)
    for t in range(TILES):
        rows = pl.ds(t * TILE, TILE)

        @pl.when(t < live[0])
        def _():
            share = 1.0 / total[t]
            for p in range(PAIRS):
                halves = [
                    acc[t, pl.ds((2 * p + h) * HEAD_DIM, HEAD_DIM)] * share[2 * p + h : 2 * p + h + 1]
                    for h in range(2)
                ]
                mixed = jnp.concatenate(halves, axis=0).astype(jnp.bfloat16)
                out[rows, pl.ds(p * TILE, TILE)] = mixed.T

        @pl.when(t >= live[0])
        def _():
            out[rows] = jnp.zeros((TILE, WIDTH), jnp.bfloat16)


def last_stage(lists, live, ids, slab, tiles, w, state):
    return pl.pallas_call(
        last_kernel,
        out_shape=jax.ShapeDtypeStruct((TILES * TILE, WIDTH), jnp.bfloat16),
        in_specs=[SMEM] * 4 + [VMEM] * 10,
        out_specs=VMEM,
        scratch_shapes=[ITEMS, pltpu.VMEM((4 * TILE, WIDTH), jnp.bfloat16), pltpu.VMEM((4 * TILE, WIDTH), jnp.bfloat16)],
        compiler_params=pltpu.CompilerParams(vmem_limit_bytes=20 << 20),
        cost_estimate=flops(8),
        name="last_stage",
    )(lists, live, ids, slab, *tiles, w, *state)


def shards(queries, keys, values, neighbours, live_tiles, boundary_ids):
    half = 2 * TILE
    slab = lax.axis_index("slab").astype(jnp.int32)[None]
    ka, kz = keys[:half], keys[half:]
    w, vt = prepare(queries, values)
    va, vz = vt[:half], vt[half:]
    near = move(keys, to_chip), move(vt, to_chip)
    cross = [move(x, to_cross) for x in (ka, va, kz, vz)]
    far_last = move(vz, to_group)
    ids = move(boundary_ids, to_group)
    far = [move(cross[i], to_forward) for i in range(3)] + [far_last]
    along = [move(cross[i], to_along) for i in range(4)]
    state = first_stage(neighbours, live_tiles, keys, vt, w)
    tiles = (*near, cross[0], cross[1], along[0], along[1], far[0], far[1])
    state = middle_stage(neighbours, live_tiles, ids, slab, tiles, w, state)
    tiles = (cross[2], cross[3], along[2], along[3], far[2], far[3])
    return last_stage(neighbours, live_tiles, ids, slab, tiles, w, state)


def solution(mesh):
    spec = P(AXES, None)
    return jax.shard_map(
        shards,
        mesh=mesh,
        in_specs=(spec, spec, spec, spec, P(AXES), spec),
        out_specs=spec,
        check_vma=False,
    )
```

```python
import functools
import math

import jax
import jax.numpy as jnp
from jax import lax
from jax.experimental import pallas as pl
from jax.experimental.pallas import tpu as pltpu
from jax.sharding import PartitionSpec as P


HEADS = 8
HEAD_DIM = 64
TILE = 128
TILES = 4
LISTED = 6
BOUNDARY = 4
EXTRA = 16
PAIRS = 4
BATCH = 4
WIDTH = HEADS * HEAD_DIM
AXES = ("group", "slab")
SCALE = HEAD_DIM ** (-0.5) * math.log2(math.e)
LOWEST = -1e30

VMEM = pl.BlockSpec(memory_space=pltpu.VMEM)
ANY = pl.BlockSpec(memory_space=pl.ANY)
SMEM = pl.BlockSpec(memory_space=pltpu.SMEM)


def move(block, target):
    groups, slabs = lax.axis_size("group"), lax.axis_size("slab")
    route = []
    for g in range(groups):
        for s in range(slabs):
            to_g, to_s = target(g, s)
            route.append((g * slabs + s, (to_g % groups) * slabs + to_s % slabs))
    return lax.ppermute(block, AXES, route)


def to_chip(g, s):
    return g, s ^ 1


def to_cross(g, s):
    return g, s ^ 3


def to_forward(g, s):
    return 1 - g, s ^ 3


def to_along(g, s):
    return g, (s + 4 if s % 2 == 0 else s - 4)


def to_group(g, s):
    return 1 - g, s


def keys_kernel(keys, first, second, sems):
    half = 2 * TILE
    copies = [
        pltpu.make_async_copy(keys.at[pl.ds(0, half)], first, sems.at[0]),
        pltpu.make_async_copy(keys.at[pl.ds(half, half)], second, sems.at[1]),
    ]
    for copy in copies:
        copy.start()
    for copy in copies:
        copy.wait()


def split_keys(keys):
    half = jax.ShapeDtypeStruct((2 * TILE, WIDTH), keys.dtype)
    return pl.pallas_call(
        keys_kernel,
        out_shape=(half, half),
        in_specs=[ANY],
        out_specs=(VMEM, VMEM),
        scratch_shapes=[pltpu.SemaphoreType.DMA((2,))],
        compiler_params=pltpu.CompilerParams(vmem_limit_bytes=2 << 20),
        cost_estimate=pl.CostEstimate(flops=400_000_000, bytes_accessed=8 << 20, transcendentals=0),
        name="split_keys",
    )(keys)


def prepare_kernel(q_ref, v_ref, ids, v_first, v_second, v_all, w_ref):
    lane = lax.broadcasted_iota(jnp.int32, (EXTRA, WIDTH), 1)
    row = jnp.zeros((EXTRA, WIDTH), jnp.int32)
    for j in range(BOUNDARY):
        row = jnp.where(lane == j, ids[0, j], row)
    v_first[2 * TILE :] = row.astype(jnp.float32).astype(jnp.bfloat16)
    for t in range(TILES):
        rows = pl.ds(t * TILE, TILE)
        part = (v_first, v_second)[t // 2]
        for p in range(PAIRS):
            lanes = pl.ds(p * TILE, TILE)
            vt = v_ref[rows, lanes].T
            v_all[rows, lanes] = vt
            part[pl.ds(t % 2 * TILE, TILE), lanes] = vt
            qt = q_ref[rows, lanes].T
            zero = jnp.zeros((HEAD_DIM, TILE), jnp.bfloat16)
            w_ref[t, p, :HEAD_DIM, :TILE] = qt[:HEAD_DIM]
            w_ref[t, p, :HEAD_DIM, TILE:] = zero
            w_ref[t, p, HEAD_DIM:, :TILE] = zero
            w_ref[t, p, HEAD_DIM:, TILE:] = qt[HEAD_DIM:]


def prepare(q, v, ids):
    half = 2 * TILE
    shapes = [(half + EXTRA, WIDTH), (half, WIDTH), v.shape, (TILES, PAIRS, TILE, 2 * TILE)]
    return pl.pallas_call(
        prepare_kernel,
        out_shape=[jax.ShapeDtypeStruct(shape, v.dtype) for shape in shapes],
        in_specs=[VMEM, VMEM, SMEM],
        out_specs=[VMEM] * 4,
        compiler_params=pltpu.CompilerParams(vmem_limit_bytes=8 << 20),
        cost_estimate=flops(1),
        name="prepare",
    )(q, v, ids)


def list_items(lists_ref, live, source_of, items):
    count = jnp.int32(0)
    for t in range(TILES):
        for j in range(LISTED):
            here, tile = source_of(lists_ref[t, j])
            items[count] = t * 16 + tile
            count = count + jnp.where(jnp.logical_and(here, t < live), 1, 0)
    for j in range(BATCH - 1):
        items[count + j] = TILES * 16
    return lax.div(count + (BATCH - 1), jnp.int32(BATCH))


def attend_items(batches, items, k_ref, v_ref, w_ref, acc, peak, total):
    def batch(b, carry):
        for u in range(BATCH):
            item = items[b * BATCH + u]
            t = lax.div(item, jnp.int32(16))
            rows = pl.ds(pl.multiple_of(lax.rem(item, jnp.int32(16)) * TILE, TILE), TILE)
            tq = jnp.minimum(t, TILES - 1)
            tops, sums, mixes = [], [], []
            for p in range(PAIRS):
                lanes = pl.ds(p * TILE, TILE)
                scores = jnp.dot(k_ref[rows, lanes], w_ref[tq, p], preferred_element_type=jnp.float32)
                top = jnp.max(scores, axis=0, keepdims=True)
                weights = jnp.exp2(scores * SCALE - top * SCALE)
                add = jnp.sum(weights, axis=0, keepdims=True)
                weights = weights.astype(jnp.bfloat16)
                vt = v_ref[rows, lanes]
                for h in range(2):
                    half = slice(h * TILE, (h + 1) * TILE)
                    tops.append(top[:, half])
                    sums.append(add[:, half])
                    mixes.append(
                        jnp.dot(
                            vt[h * HEAD_DIM : (h + 1) * HEAD_DIM],
                            weights[:, half],
                            preferred_element_type=jnp.float32,
                        )
                    )
            top = jnp.concatenate(tops, axis=0)
            add = jnp.concatenate(sums, axis=0)
            old = peak[t]
            new = jnp.maximum(old, top)
            keep = jnp.exp2((old - new) * SCALE)
            take = jnp.exp2((top - new) * SCALE)
            peak[t] = new
            total[t] = total[t] * keep + add * take
            for h in range(HEADS):
                dims = pl.ds(h * HEAD_DIM, HEAD_DIM)
                acc[t, dims] = acc[t, dims] * keep[h : h + 1] + mixes[h] * take[h : h + 1]
        return carry

    lax.fori_loop(0, batches, batch, 0)


def first_kernel(lists, live, k_ref, v_ref, w_ref, acc, peak, total, items):
    acc[...] = jnp.zeros_like(acc)
    peak[...] = jnp.full_like(peak, LOWEST)
    total[...] = jnp.zeros_like(total)
    batches = list_items(lists, live[0], lambda pos: (pos < TILES, lax.rem(pos, 4)), items)
    attend_items(batches, items, k_ref, v_ref, w_ref, acc, peak, total)


STATE = (
    jax.ShapeDtypeStruct((TILES + 1, WIDTH, TILE), jnp.float32),
    jax.ShapeDtypeStruct((TILES + 1, HEADS, TILE), jnp.float32),
    jax.ShapeDtypeStruct((TILES + 1, HEADS, TILE), jnp.float32),
)
ITEMS = pltpu.SMEM((TILES * LISTED + BATCH,), jnp.int32)


def flops(items):
    return pl.CostEstimate(flops=items * 40_000_000, bytes_accessed=1 << 20, transcendentals=0)


def first_stage(lists, live, k, v, w):
    return pl.pallas_call(
        first_kernel,
        out_shape=STATE,
        in_specs=[SMEM, SMEM] + [VMEM] * 3,
        out_specs=(VMEM,) * 3,
        scratch_shapes=[ITEMS],
        compiler_params=pltpu.CompilerParams(vmem_limit_bytes=16 << 20),
        cost_estimate=flops(8),
        name="first_stage",
    )(lists, live, k, v, w)


def is_inner():
    at = lax.rem(lax.axis_index("slab"), 4)
    return jnp.logical_or(at == 1, at == 2)


def is_odd():
    return lax.rem(lax.axis_index("slab"), 2) == 1


def find_near():
    base = jnp.where(is_odd(), TILES, 2 * TILES)

    def find(pos):
        at = pos - base
        here = jnp.logical_and(at >= 0, at < TILES)
        return here, jnp.where(here, at, 0)

    return find


def find_other(half):
    base = jnp.where(is_odd(), 2 * TILES, TILES) + 2 * half

    def find(pos):
        at = pos - base
        here = jnp.logical_and(at >= 0, at < 2)
        return here, jnp.where(here, at, 0)

    return find


def find_far(marks, half):
    lane = lax.broadcasted_iota(jnp.int32, (1, TILE), 1)
    line = marks[2 * TILE : 2 * TILE + EXTRA, :TILE].astype(jnp.float32)[:1]
    ids = [jnp.sum(jnp.where(lane == j, line, 0.0)).astype(jnp.int32) for j in range(BOUNDARY)]

    def find(pos):
        at = jnp.int32(-1)
        for j in range(BOUNDARY):
            at = jnp.where(pos == 3 * TILES + j, ids[j] - 2 * half, at)
        here = jnp.logical_and(at >= 0, at < 2)
        return here, jnp.where(here, at, 0)

    return find


def near_kernel(lists, live, k_ref, v_ref, w_ref, acc0, peak0, total0, acc, peak, total, items):
    batches = list_items(lists, live[0], find_near(), items)
    attend_items(batches, items, k_ref, v_ref, w_ref, acc, peak, total)


def other_kernel(half, lists, live, kb, vb, kd, vd, w_ref, acc0, peak0, total0, acc, peak, total, items):
    batches = list_items(lists, live[0], find_other(half), items)

    @pl.when(is_inner())
    def _():
        attend_items(batches, items, kb, vb, w_ref, acc, peak, total)

    @pl.when(jnp.logical_not(is_inner()))
    def _():
        attend_items(batches, items, kd, vd, w_ref, acc, peak, total)


def far_kernel(lists, live, k_ref, v_ref, w_ref, acc0, peak0, total0, acc, peak, total, items):
    batches = list_items(lists, live[0], find_far(v_ref, 0), items)
    attend_items(batches, items, k_ref, v_ref, w_ref, acc, peak, total)


def stage(kernel, lists, live, tiles, w, state):
    args = (lists, live, *tiles, w, *state)
    first = len(args) - 3
    return pl.pallas_call(
        kernel,
        out_shape=STATE,
        in_specs=[SMEM] * 2 + [VMEM] * (len(args) - 2),
        out_specs=(VMEM,) * 3,
        input_output_aliases={first: 0, first + 1: 1, first + 2: 2},
        scratch_shapes=[ITEMS],
        compiler_params=pltpu.CompilerParams(vmem_limit_bytes=12 << 20),
        cost_estimate=flops(8),
    )(*args)


def last_kernel(lists, live, marks, k_ref, v_ref, w_ref, acc, peak, total, out, items):
    batches = list_items(lists, live[0], find_far(marks, 1), items)
    attend_items(batches, items, k_ref, v_ref, w_ref, acc, peak, total)
    for t in range(TILES):
        rows = pl.ds(t * TILE, TILE)

        @pl.when(t < live[0])
        def _():
            share = 1.0 / total[t]
            for p in range(PAIRS):
                halves = [
                    acc[t, pl.ds((2 * p + h) * HEAD_DIM, HEAD_DIM)] * share[2 * p + h : 2 * p + h + 1]
                    for h in range(2)
                ]
                mixed = jnp.concatenate(halves, axis=0).astype(jnp.bfloat16)
                out[rows, pl.ds(p * TILE, TILE)] = mixed.T

        @pl.when(t >= live[0])
        def _():
            out[rows] = jnp.zeros((TILE, WIDTH), jnp.bfloat16)


def last_stage(lists, live, tiles, w, state):
    return pl.pallas_call(
        last_kernel,
        out_shape=jax.ShapeDtypeStruct((TILES * TILE, WIDTH), jnp.bfloat16),
        in_specs=[SMEM] * 2 + [VMEM] * 7,
        out_specs=VMEM,
        scratch_shapes=[ITEMS],
        compiler_params=pltpu.CompilerParams(vmem_limit_bytes=12 << 20),
        cost_estimate=flops(8),
        name="last_stage",
    )(lists, live, *tiles, w, *state)


def shards(queries, keys, values, neighbours, live_tiles, boundary_ids):
    ka, kz = split_keys(keys)
    va, vz, vt, w = prepare(queries, values, boundary_ids)
    near = move(keys, to_chip), move(vt, to_chip)
    cross = [move(x, to_cross) for x in (ka, va, kz, vz)]
    far_last = move(vz, to_group)
    far = [move(cross[i], to_forward) for i in range(3)] + [far_last]
    along = [move(cross[i], to_along) for i in range(4)]
    common = neighbours, live_tiles
    state = first_stage(neighbours, live_tiles, keys, vt, w)
    state = stage(near_kernel, *common, near, w, state)
    tiles = cross[0], cross[1], along[0], along[1]
    state = stage(functools.partial(other_kernel, 0), *common, tiles, w, state)
    state = stage(far_kernel, *common, (far[0], far[1]), w, state)
    tiles = cross[2], cross[3], along[2], along[3]
    state = stage(functools.partial(other_kernel, 1), *common, tiles, w, state)
    return last_stage(neighbours, live_tiles, (far[1], far[2], far[3]), w, state)


def solution(mesh):
    spec = P(AXES, None)
    return jax.shard_map(
        shards,
        mesh=mesh,
        in_specs=(spec, spec, spec, spec, P(AXES), spec),
        out_specs=spec,
        check_vma=False,
    )
```

```python
import math

import jax
import jax.numpy as jnp
from jax import lax
from jax.experimental import pallas as pl
from jax.experimental.pallas import tpu as pltpu
from jax.sharding import PartitionSpec as P


HEADS = 8
HEAD_DIM = 64
TILE = 128
TILES = 4
LISTED = 6
BOUNDARY = 4
EXTRA = 16
PAIRS = 4
BATCH = 4
WIDTH = HEADS * HEAD_DIM
AXES = ("group", "slab")
SCALE = HEAD_DIM ** (-0.5) * math.log2(math.e)
LOWEST = -1e30

VMEM = pl.BlockSpec(memory_space=pltpu.VMEM)
ANY = pl.BlockSpec(memory_space=pl.ANY)
SMEM = pl.BlockSpec(memory_space=pltpu.SMEM)


def move(block, target):
    groups, slabs = lax.axis_size("group"), lax.axis_size("slab")
    route = []
    for g in range(groups):
        for s in range(slabs):
            to_g, to_s = target(g, s)
            route.append((g * slabs + s, (to_g % groups) * slabs + to_s % slabs))
    return lax.ppermute(block, AXES, route)


def to_chip(g, s):
    return g, s ^ 1


def to_cross(g, s):
    return g, s ^ 3


def to_forward(g, s):
    return 1 - g, s ^ 3


def to_along(g, s):
    return g, (s + 4 if s % 2 == 0 else s - 4)


def to_other(g, s):
    return g, (s - 1 if s % 2 == 0 else s + 1)


def keys_kernel(keys, *refs):
    *chunks, sems = refs
    copies = [
        pltpu.make_async_copy(keys.at[pl.ds(start, chunk.shape[0])], chunk, sems.at[i])
        for i, (start, chunk) in enumerate(zip((0, TILE, 2 * TILE), chunks))
    ]
    for copy in copies:
        copy.start()
    for copy in copies:
        copy.wait()


def split_keys(keys):
    return pl.pallas_call(
        keys_kernel,
        out_shape=[jax.ShapeDtypeStruct((n * TILE, WIDTH), keys.dtype) for n in (1, 1, 2)],
        in_specs=[ANY],
        out_specs=[VMEM] * 3,
        scratch_shapes=[pltpu.SemaphoreType.DMA((3,))],
        compiler_params=pltpu.CompilerParams(vmem_limit_bytes=2 << 20),
        cost_estimate=pl.CostEstimate(flops=400_000_000, bytes_accessed=8 << 20, transcendentals=0),
        name="split_keys",
    )(keys)


def prepare_kernel(q_ref, v_ref, ids, v_first, v_second, v_all, w_ref):
    lane = lax.broadcasted_iota(jnp.int32, (EXTRA, WIDTH), 1)
    row = jnp.zeros((EXTRA, WIDTH), jnp.int32)
    for j in range(BOUNDARY):
        row = jnp.where(lane == j, ids[0, j], row)
    v_first[2 * TILE :] = row.astype(jnp.float32).astype(jnp.bfloat16)
    for t in range(TILES):
        rows = pl.ds(t * TILE, TILE)
        part = (v_first, v_second)[t // 2]
        for p in range(PAIRS):
            lanes = pl.ds(p * TILE, TILE)
            vt = v_ref[rows, lanes].T
            v_all[rows, lanes] = vt
            part[pl.ds(t % 2 * TILE, TILE), lanes] = vt
            qt = q_ref[rows, lanes].T
            zero = jnp.zeros((HEAD_DIM, TILE), jnp.bfloat16)
            w_ref[t, p, :HEAD_DIM, :TILE] = qt[:HEAD_DIM]
            w_ref[t, p, :HEAD_DIM, TILE:] = zero
            w_ref[t, p, HEAD_DIM:, :TILE] = zero
            w_ref[t, p, HEAD_DIM:, TILE:] = qt[HEAD_DIM:]


def prepare(q, v, ids):
    half = 2 * TILE
    shapes = [(half + EXTRA, WIDTH), (half, WIDTH), v.shape, (TILES, PAIRS, TILE, 2 * TILE)]
    return pl.pallas_call(
        prepare_kernel,
        out_shape=[jax.ShapeDtypeStruct(shape, v.dtype) for shape in shapes],
        in_specs=[VMEM, VMEM, SMEM],
        out_specs=[VMEM] * 4,
        compiler_params=pltpu.CompilerParams(vmem_limit_bytes=8 << 20),
        cost_estimate=flops(1),
        name="prepare",
    )(q, v, ids)


def list_items(lists_ref, live, source_of, items):
    count = jnp.int32(0)
    for t in range(TILES):
        for j in range(LISTED):
            here, tile = source_of(lists_ref[t, j])
            items[count] = t * 16 + tile
            count = count + jnp.where(jnp.logical_and(here, t < live), 1, 0)
    for j in range(BATCH - 1):
        items[count + j] = TILES * 16
    return count


def attend_batch(first, size, items, k_ref, v_ref, w_ref, acc, peak, total):
    for u in range(size):
        item = items[first + u]
        t = lax.div(item, jnp.int32(16))
        rows = pl.ds(pl.multiple_of(lax.rem(item, jnp.int32(16)) * TILE, TILE), TILE)
        tq = jnp.minimum(t, TILES - 1)
        tops, sums, mixes = [], [], []
        for p in range(PAIRS):
            lanes = pl.ds(p * TILE, TILE)
            scores = jnp.dot(k_ref[rows, lanes], w_ref[tq, p], preferred_element_type=jnp.float32)
            top = jnp.max(scores, axis=0, keepdims=True)
            weights = jnp.exp2(scores * SCALE - top * SCALE)
            add = jnp.sum(weights, axis=0, keepdims=True)
            weights = weights.astype(jnp.bfloat16)
            vt = v_ref[rows, lanes]
            for h in range(2):
                half = slice(h * TILE, (h + 1) * TILE)
                tops.append(top[:, half])
                sums.append(add[:, half])
                mixes.append(
                    jnp.dot(
                        vt[h * HEAD_DIM : (h + 1) * HEAD_DIM],
                        weights[:, half],
                        preferred_element_type=jnp.float32,
                    )
                )
        top = jnp.concatenate(tops, axis=0)
        add = jnp.concatenate(sums, axis=0)
        old = peak[t]
        new = jnp.maximum(old, top)
        keep = jnp.exp2((old - new) * SCALE)
        take = jnp.exp2((top - new) * SCALE)
        peak[t] = new
        total[t] = total[t] * keep + add * take
        for h in range(HEADS):
            dims = pl.ds(h * HEAD_DIM, HEAD_DIM)
            acc[t, dims] = acc[t, dims] * keep[h : h + 1] + mixes[h] * take[h : h + 1]


def attend_items(count, items, *refs):
    whole = lax.div(count + (BATCH // 2 - 1), jnp.int32(BATCH))

    def batch(b, carry):
        attend_batch(b * BATCH, BATCH, items, *refs)
        return carry

    lax.fori_loop(0, whole, batch, 0)

    @pl.when(count > whole * BATCH)
    def _():
        attend_batch(whole * BATCH, BATCH // 2, items, *refs)


def first_kernel(lists, live, k_ref, v_ref, b0, b1, w_ref, acc, peak, total, joined, items):
    joined[:TILE] = b0[...]
    joined[TILE:] = b1[...]
    acc[...] = jnp.zeros_like(acc)
    peak[...] = jnp.full_like(peak, LOWEST)
    total[...] = jnp.zeros_like(total)
    count = list_items(lists, live[0], lambda pos: (pos < TILES, lax.rem(pos, 4)), items)
    attend_items(count, items, k_ref, v_ref, w_ref, acc, peak, total)


STATE = (
    jax.ShapeDtypeStruct((TILES + 1, WIDTH, TILE), jnp.float32),
    jax.ShapeDtypeStruct((TILES + 1, HEADS, TILE), jnp.float32),
    jax.ShapeDtypeStruct((TILES + 1, HEADS, TILE), jnp.float32),
)
ITEMS = pltpu.SMEM((TILES * LISTED + BATCH,), jnp.int32)


def flops(items):
    return pl.CostEstimate(flops=items * 40_000_000, bytes_accessed=1 << 20, transcendentals=0)


def first_stage(lists, live, k, v, b0, b1, w):
    return pl.pallas_call(
        first_kernel,
        out_shape=STATE + (jax.ShapeDtypeStruct((2 * TILE, WIDTH), k.dtype),),
        in_specs=[SMEM, SMEM] + [VMEM] * 5,
        out_specs=(VMEM,) * 4,
        scratch_shapes=[ITEMS],
        compiler_params=pltpu.CompilerParams(vmem_limit_bytes=16 << 20),
        cost_estimate=flops(8),
        name="first_stage",
    )(lists, live, k, v, b0, b1, w)


def is_inner():
    at = lax.rem(lax.axis_index("slab"), 4)
    return jnp.logical_or(at == 1, at == 2)


def is_odd():
    return lax.rem(lax.axis_index("slab"), 2) == 1


def find_near():
    base = jnp.where(is_odd(), TILES, 2 * TILES)

    def find(pos):
        at = pos - base
        here = jnp.logical_and(at >= 0, at < TILES)
        return here, jnp.where(here, at, 0)

    return find


def find_other(half):
    base = jnp.where(is_odd(), 2 * TILES, TILES) + 2 * half

    def find(pos):
        at = pos - base
        here = jnp.logical_and(at >= 0, at < 2)
        return here, jnp.where(here, at, 0)

    return find


def find_far(marks, half):
    lane = lax.broadcasted_iota(jnp.int32, (1, TILE), 1)
    line = marks[2 * TILE : 2 * TILE + EXTRA, :TILE].astype(jnp.float32)[:1]
    ids = [jnp.sum(jnp.where(lane == j, line, 0.0)).astype(jnp.int32) for j in range(BOUNDARY)]

    def find(pos):
        at = jnp.int32(-1)
        for j in range(BOUNDARY):
            at = jnp.where(pos == 3 * TILES + j, ids[j] - 2 * half, at)
        here = jnp.logical_and(at >= 0, at < 2)
        return here, jnp.where(here, at, 0)

    return find


def near_kernel(lists, live, k_ref, v_ref, w_ref, acc0, peak0, total0, acc, peak, total, items):
    count = list_items(lists, live[0], find_near(), items)
    attend_items(count, items, k_ref, v_ref, w_ref, acc, peak, total)


def attend_other(half, lists, live, kb, vb, kd, vd, w_ref, acc, peak, total, items):
    count = list_items(lists, live[0], find_other(half), items)

    @pl.when(is_inner())
    def _():
        attend_items(count, items, kb, vb, w_ref, acc, peak, total)

    @pl.when(jnp.logical_not(is_inner()))
    def _():
        attend_items(count, items, kd, vd, w_ref, acc, peak, total)


def attend_far(half, marks, lists, live, k_ref, v_ref, w_ref, acc, peak, total, items):
    count = list_items(lists, live[0], find_far(marks, half), items)
    attend_items(count, items, k_ref, v_ref, w_ref, acc, peak, total)


def middle_kernel(lists, live, kb, vb, kd, vd, kc0, kc1, vc, w_ref, acc0, peak0, total0, acc, peak, total, items, kc):
    kc[:TILE] = kc0[...]
    kc[TILE:] = kc1[...]
    attend_far(0, vc, lists, live, kc, vc, w_ref, acc, peak, total, items)
    attend_other(0, lists, live, kb, vb, kd, vd, w_ref, acc, peak, total, items)


def stage(kernel, lists, live, tiles, w, state, extra=(), scratch=()):
    args = (lists, live, *tiles, w, *state)
    first = len(args) - 3
    return pl.pallas_call(
        kernel,
        out_shape=STATE + tuple(extra),
        in_specs=[SMEM] * 2 + [VMEM] * (len(args) - 2),
        out_specs=(VMEM,) * (3 + len(extra)),
        input_output_aliases={first: 0, first + 1: 1, first + 2: 2},
        scratch_shapes=[ITEMS, *scratch],
        compiler_params=pltpu.CompilerParams(vmem_limit_bytes=12 << 20),
        cost_estimate=flops(8),
    )(*args)


def last_kernel(lists, live, marks, kb, vb, kd, vd, kc, vc, w_ref, acc, peak, total, out, items):
    attend_far(1, marks, lists, live, kc, vc, w_ref, acc, peak, total, items)
    attend_other(1, lists, live, kb, vb, kd, vd, w_ref, acc, peak, total, items)
    for t in range(TILES):
        rows = pl.ds(t * TILE, TILE)

        @pl.when(t < live[0])
        def _():
            share = 1.0 / total[t]
            for p in range(PAIRS):
                halves = [
                    acc[t, pl.ds((2 * p + h) * HEAD_DIM, HEAD_DIM)] * share[2 * p + h : 2 * p + h + 1]
                    for h in range(2)
                ]
                mixed = jnp.concatenate(halves, axis=0).astype(jnp.bfloat16)
                out[rows, pl.ds(p * TILE, TILE)] = mixed.T

        @pl.when(t >= live[0])
        def _():
            out[rows] = jnp.zeros((TILE, WIDTH), jnp.bfloat16)


def last_stage(lists, live, tiles, w, state):
    return pl.pallas_call(
        last_kernel,
        out_shape=jax.ShapeDtypeStruct((TILES * TILE, WIDTH), jnp.bfloat16),
        in_specs=[SMEM] * 2 + [VMEM] * 11,
        out_specs=VMEM,
        scratch_shapes=[ITEMS],
        compiler_params=pltpu.CompilerParams(vmem_limit_bytes=12 << 20),
        cost_estimate=flops(8),
        name="last_stage",
    )(lists, live, *tiles, w, *state)


def shards(queries, keys, values, neighbours, live_tiles, boundary_ids):
    keys_in = split_keys(keys)
    va, vz, vt, w = prepare(queries, values, boundary_ids)
    common = neighbours, live_tiles
    pair = jax.ShapeDtypeStruct((2 * TILE, WIDTH), keys.dtype)
    near = move(keys, to_chip), move(vt, to_chip)
    k0, k1, kz = keys_in
    cross = [move(x, to_cross) for x in (k0, k1, va, vz)]
    far = [move(x, to_forward) for x in cross]
    far_last = move(move(kz, to_forward), to_cross)
    other_last = move(kz, to_other)
    *state, joined = first_stage(*common, keys, vt, cross[0], cross[1], w)
    state = stage(near_kernel, *common, near, w, state)
    along = [move(x, to_along) for x in (joined, cross[2], cross[3])]
    tiles = joined, cross[2], along[0], along[1], far[0], far[1], far[2]
    scratch = (pltpu.VMEM(pair.shape, pair.dtype),)
    state = stage(middle_kernel, *common, tiles, w, state, scratch=scratch)
    tiles = far[2], other_last, cross[3], other_last, along[2], far_last, far[3]
    return last_stage(*common, tiles, w, state)


def solution(mesh):
    spec = P(AXES, None)
    return jax.shard_map(
        shards,
        mesh=mesh,
        in_specs=(spec, spec, spec, spec, P(AXES), spec),
        out_specs=spec,
        check_vma=False,
    )
```

```python
import math

import jax
import jax.numpy as jnp
from jax import lax
from jax.experimental import pallas as pl
from jax.experimental.pallas import tpu as pltpu
from jax.sharding import PartitionSpec as P


HEADS = 8
HEAD_DIM = 64
TILE = 128
TILES = 4
LISTED = 6
BOUNDARY = 4
EXTRA = 16
PAIRS = 4
BATCH = 4
WIDTH = HEADS * HEAD_DIM
AXES = ("group", "slab")
SCALE = HEAD_DIM ** (-0.5) * math.log2(math.e)
LOWEST = -1e30

VMEM = pl.BlockSpec(memory_space=pltpu.VMEM)
ANY = pl.BlockSpec(memory_space=pl.ANY)
SMEM = pl.BlockSpec(memory_space=pltpu.SMEM)


def move(block, target):
    groups, slabs = lax.axis_size("group"), lax.axis_size("slab")
    route = []
    for g in range(groups):
        for s in range(slabs):
            to_g, to_s = target(g, s)
            route.append((g * slabs + s, (to_g % groups) * slabs + to_s % slabs))
    return lax.ppermute(block, AXES, route)


def to_chip(g, s):
    return g, s ^ 1


def to_cross(g, s):
    return g, s ^ 3


def to_forward(g, s):
    return 1 - g, s ^ 3


def to_along(g, s):
    return g, (s + 4 if s % 2 == 0 else s - 4)


def to_other(g, s):
    return g, (s - 1 if s % 2 == 0 else s + 1)


def keys_kernel(keys, *refs):
    *chunks, sems = refs
    copies = [
        pltpu.make_async_copy(keys.at[pl.ds(start, chunk.shape[0])], chunk, sems.at[i])
        for i, (start, chunk) in enumerate(zip((0, TILE, 2 * TILE), chunks))
    ]
    for copy in copies:
        copy.start()
    for copy in copies:
        copy.wait()


def split_keys(keys):
    return pl.pallas_call(
        keys_kernel,
        out_shape=[jax.ShapeDtypeStruct((n * TILE, WIDTH), keys.dtype) for n in (1, 1, 2)],
        in_specs=[ANY],
        out_specs=[VMEM] * 3,
        scratch_shapes=[pltpu.SemaphoreType.DMA((3,))],
        compiler_params=pltpu.CompilerParams(vmem_limit_bytes=2 << 20),
        cost_estimate=pl.CostEstimate(flops=400_000_000, bytes_accessed=8 << 20, transcendentals=0),
        name="split_keys",
    )(keys)


def prepare_kernel(q_ref, v_ref, ids, v_first, v_second, v_all, w_ref):
    lane = lax.broadcasted_iota(jnp.int32, (EXTRA, WIDTH), 1)
    row = jnp.zeros((EXTRA, WIDTH), jnp.int32)
    for j in range(BOUNDARY):
        row = jnp.where(lane == j, ids[0, j], row)
    v_first[2 * TILE :] = row.astype(jnp.float32).astype(jnp.bfloat16)
    for t in range(TILES):
        rows = pl.ds(t * TILE, TILE)
        part = (v_first, v_second)[t // 2]
        for p in range(PAIRS):
            lanes = pl.ds(p * TILE, TILE)
            vt = v_ref[rows, lanes].T
            v_all[rows, lanes] = vt
            part[pl.ds(t % 2 * TILE, TILE), lanes] = vt
            qt = q_ref[rows, lanes].T
            zero = jnp.zeros((HEAD_DIM, TILE), jnp.bfloat16)
            w_ref[t, p, :HEAD_DIM, :TILE] = qt[:HEAD_DIM]
            w_ref[t, p, :HEAD_DIM, TILE:] = zero
            w_ref[t, p, HEAD_DIM:, :TILE] = zero
            w_ref[t, p, HEAD_DIM:, TILE:] = qt[HEAD_DIM:]


def prepare(q, v, ids):
    half = 2 * TILE
    shapes = [(half + EXTRA, WIDTH), (half, WIDTH), v.shape, (TILES, PAIRS, TILE, 2 * TILE)]
    return pl.pallas_call(
        prepare_kernel,
        out_shape=[jax.ShapeDtypeStruct(shape, v.dtype) for shape in shapes],
        in_specs=[VMEM, VMEM, SMEM],
        out_specs=[VMEM] * 4,
        compiler_params=pltpu.CompilerParams(vmem_limit_bytes=8 << 20),
        cost_estimate=flops(1),
        name="prepare",
    )(q, v, ids)


def list_items(lists_ref, live, source_of, items):
    count = jnp.int32(0)
    for t in range(TILES):
        for j in range(LISTED):
            here, tile = source_of(lists_ref[t, j])
            items[count] = t * 16 + tile
            count = count + jnp.where(jnp.logical_and(here, t < live), 1, 0)
    for j in range(BATCH - 1):
        items[count + j] = TILES * 16
    return count


def attend_batch(first, size, items, k_ref, v_ref, w_ref, acc, peak, total):
    for u in range(size):
        item = items[first + u]
        t = lax.div(item, jnp.int32(16))
        rows = pl.ds(pl.multiple_of(lax.rem(item, jnp.int32(16)) * TILE, TILE), TILE)
        tq = jnp.minimum(t, TILES - 1)
        tops, sums, mixes = [], [], []
        for p in range(PAIRS):
            lanes = pl.ds(p * TILE, TILE)
            scores = jnp.dot(k_ref[rows, lanes], w_ref[tq, p], preferred_element_type=jnp.float32)
            top = jnp.max(scores, axis=0, keepdims=True)
            weights = jnp.exp2(scores * SCALE - top * SCALE)
            add = jnp.sum(weights, axis=0, keepdims=True)
            weights = weights.astype(jnp.bfloat16)
            vt = v_ref[rows, lanes]
            for h in range(2):
                half = slice(h * TILE, (h + 1) * TILE)
                tops.append(top[:, half])
                sums.append(add[:, half])
                mixes.append(
                    jnp.dot(
                        vt[h * HEAD_DIM : (h + 1) * HEAD_DIM],
                        weights[:, half],
                        preferred_element_type=jnp.float32,
                    )
                )
        top = jnp.concatenate(tops, axis=0)
        add = jnp.concatenate(sums, axis=0)
        old = peak[t]
        new = jnp.maximum(old, top)
        keep = jnp.exp2((old - new) * SCALE)
        take = jnp.exp2((top - new) * SCALE)
        peak[t] = new
        total[t] = total[t] * keep + add * take
        for h in range(HEADS):
            dims = pl.ds(h * HEAD_DIM, HEAD_DIM)
            acc[t, dims] = acc[t, dims] * keep[h : h + 1] + mixes[h] * take[h : h + 1]


def attend_items(count, items, *refs):
    whole = lax.div(count + (BATCH // 2 - 1), jnp.int32(BATCH))

    def batch(b, carry):
        attend_batch(b * BATCH, BATCH, items, *refs)
        return carry

    lax.fori_loop(0, whole, batch, 0)

    @pl.when(count > whole * BATCH)
    def _():
        attend_batch(whole * BATCH, BATCH // 2, items, *refs)


def first_kernel(lists, live, k_ref, v_ref, b0, b1, w_ref, acc, peak, total, joined, items):
    joined[:TILE] = b0[...]
    joined[TILE:] = b1[...]
    acc[...] = jnp.zeros_like(acc)
    peak[...] = jnp.full_like(peak, LOWEST)
    total[...] = jnp.zeros_like(total)
    count = list_items(lists, live[0], lambda pos: (pos < TILES, lax.rem(pos, 4)), items)
    attend_items(count, items, k_ref, v_ref, w_ref, acc, peak, total)


STATE = (
    jax.ShapeDtypeStruct((TILES + 1, WIDTH, TILE), jnp.float32),
    jax.ShapeDtypeStruct((TILES + 1, HEADS, TILE), jnp.float32),
    jax.ShapeDtypeStruct((TILES + 1, HEADS, TILE), jnp.float32),
)
ITEMS = pltpu.SMEM((TILES * LISTED + BATCH,), jnp.int32)


def flops(items):
    return pl.CostEstimate(flops=items * 40_000_000, bytes_accessed=1 << 20, transcendentals=0)


def first_stage(lists, live, k, v, b0, b1, w):
    return pl.pallas_call(
        first_kernel,
        out_shape=STATE + (jax.ShapeDtypeStruct((2 * TILE, WIDTH), k.dtype),),
        in_specs=[SMEM, SMEM] + [VMEM] * 5,
        out_specs=(VMEM,) * 4,
        scratch_shapes=[ITEMS],
        compiler_params=pltpu.CompilerParams(vmem_limit_bytes=16 << 20),
        cost_estimate=flops(8),
        name="first_stage",
    )(lists, live, k, v, b0, b1, w)


def is_inner():
    at = lax.rem(lax.axis_index("slab"), 4)
    return jnp.logical_or(at == 1, at == 2)


def is_odd():
    return lax.rem(lax.axis_index("slab"), 2) == 1


def find_near():
    base = jnp.where(is_odd(), TILES, 2 * TILES)

    def find(pos):
        at = pos - base
        here = jnp.logical_and(at >= 0, at < TILES)
        return here, jnp.where(here, at, 0)

    return find


def find_other(half):
    base = jnp.where(is_odd(), 2 * TILES, TILES) + 2 * half

    def find(pos):
        at = pos - base
        here = jnp.logical_and(at >= 0, at < 2)
        return here, jnp.where(here, at, 0)

    return find


def find_far(marks, half):
    lane = lax.broadcasted_iota(jnp.int32, (1, TILE), 1)
    line = marks[2 * TILE : 2 * TILE + EXTRA, :TILE].astype(jnp.float32)[:1]
    ids = [jnp.sum(jnp.where(lane == j, line, 0.0)).astype(jnp.int32) for j in range(BOUNDARY)]

    def find(pos):
        at = jnp.int32(-1)
        for j in range(BOUNDARY):
            at = jnp.where(pos == 3 * TILES + j, ids[j] - 2 * half, at)
        here = jnp.logical_and(at >= 0, at < 2)
        return here, jnp.where(here, at, 0)

    return find


def near_kernel(lists, live, k_ref, v_ref, w_ref, acc0, peak0, total0, acc, peak, total, items):
    count = list_items(lists, live[0], find_near(), items)
    attend_items(count, items, k_ref, v_ref, w_ref, acc, peak, total)


def attend_other(half, lists, live, kb, vb, kd, vd, w_ref, acc, peak, total, items):
    count = list_items(lists, live[0], find_other(half), items)

    @pl.when(is_inner())
    def _():
        attend_items(count, items, kb, vb, w_ref, acc, peak, total)

    @pl.when(jnp.logical_not(is_inner()))
    def _():
        attend_items(count, items, kd, vd, w_ref, acc, peak, total)


def attend_far(half, marks, lists, live, k_ref, v_ref, w_ref, acc, peak, total, items):
    count = list_items(lists, live[0], find_far(marks, half), items)
    attend_items(count, items, k_ref, v_ref, w_ref, acc, peak, total)


def middle_kernel(lists, live, kb, vb, kd, vd, kc0, kc1, vc, w_ref, acc0, peak0, total0, acc, peak, total, items, kc):
    kc[:TILE] = kc0[...]
    kc[TILE:] = kc1[...]
    attend_far(0, vc, lists, live, kc, vc, w_ref, acc, peak, total, items)
    attend_other(0, lists, live, kb, vb, kd, vd, w_ref, acc, peak, total, items)


def stage(kernel, lists, live, tiles, w, state, extra=(), scratch=()):
    args = (lists, live, *tiles, w, *state)
    first = len(args) - 3
    return pl.pallas_call(
        kernel,
        out_shape=STATE + tuple(extra),
        in_specs=[SMEM] * 2 + [VMEM] * (len(args) - 2),
        out_specs=(VMEM,) * (3 + len(extra)),
        input_output_aliases={first: 0, first + 1: 1, first + 2: 2},
        scratch_shapes=[ITEMS, *scratch],
        compiler_params=pltpu.CompilerParams(vmem_limit_bytes=12 << 20),
        cost_estimate=flops(8),
    )(*args)


def far_kernel(lists, live, marks, kc, vc, w_ref, acc0, peak0, total0, acc, peak, total, items):
    attend_far(1, marks, lists, live, kc, vc, w_ref, acc, peak, total, items)


def last_kernel(lists, live, kb, vb, kd, vd, w_ref, acc, peak, total, out, items, done, sems):
    attend_other(1, lists, live, kb, vb, kd, vd, w_ref, acc, peak, total, items)
    copies = []
    for t in range(TILES):
        rows = pl.ds(t * TILE, TILE)
        share = jnp.where(t < live[0], 1.0 / total[t], 0.0)
        for p in range(PAIRS):
            halves = [
                acc[t, pl.ds((2 * p + h) * HEAD_DIM, HEAD_DIM)] * share[2 * p + h : 2 * p + h + 1]
                for h in range(2)
            ]
            mixed = jnp.concatenate(halves, axis=0).astype(jnp.bfloat16)
            done[rows, pl.ds(p * TILE, TILE)] = mixed.T
        copies.append(pltpu.make_async_copy(done.at[rows], out.at[rows], sems.at[t]))
        copies[-1].start()
    for copy in copies:
        copy.wait()


def last_stage(lists, live, tiles, w, state):
    return pl.pallas_call(
        last_kernel,
        out_shape=jax.ShapeDtypeStruct((TILES * TILE, WIDTH), jnp.bfloat16),
        in_specs=[SMEM] * 2 + [VMEM] * 8,
        out_specs=ANY,
        scratch_shapes=[ITEMS, pltpu.VMEM((TILES * TILE, WIDTH), jnp.bfloat16), pltpu.SemaphoreType.DMA((TILES,))],
        compiler_params=pltpu.CompilerParams(vmem_limit_bytes=12 << 20),
        cost_estimate=flops(8),
        name="last_stage",
    )(lists, live, *tiles, w, *state)


def shards(queries, keys, values, neighbours, live_tiles, boundary_ids):
    keys_in = split_keys(keys)
    va, vz, vt, w = prepare(queries, values, boundary_ids)
    common = neighbours, live_tiles
    pair = jax.ShapeDtypeStruct((2 * TILE, WIDTH), keys.dtype)
    near = move(keys, to_chip), move(vt, to_chip)
    k0, k1, kz = keys_in
    cross = [move(x, to_cross) for x in (k0, k1, va, vz)]
    far = [move(x, to_forward) for x in cross]
    far_last = move(move(kz, to_forward), to_cross)
    other_last = move(kz, to_other)
    *state, joined = first_stage(*common, keys, vt, cross[0], cross[1], w)
    state = stage(near_kernel, *common, near, w, state)
    along = [move(x, to_along) for x in (joined, cross[2], cross[3])]
    tiles = joined, cross[2], along[0], along[1], far[0], far[1], far[2]
    scratch = (pltpu.VMEM(pair.shape, pair.dtype),)
    state = stage(middle_kernel, *common, tiles, w, state, scratch=scratch)
    state = stage(far_kernel, *common, (far[2], far_last, far[3]), w, state)
    tiles = other_last, cross[3], other_last, along[2]
    return last_stage(*common, tiles, w, state)


def solution(mesh):
    spec = P(AXES, None)
    return jax.shard_map(
        shards,
        mesh=mesh,
        in_specs=(spec, spec, spec, spec, P(AXES), spec),
        out_specs=spec,
        check_vma=False,
    )
```
